32 devices in a mesh: seq: 16 (over z, y, core), tensor: 2 (over x).
Axes of the slice: x: 2, y: 2, z: 4, core: 2. Of those that a mesh axis runs over, the one named last changes fastest.
Arguments:
- hidden: bfloat16 [1024, 7168], P('seq', 'tensor'), may hold values from -200 to 200
- attn_gain: float32 [7168], P('tensor'), may hold values from 0.25 to 1.75
- kv_down: bfloat16 [7168, 576], P('tensor'), may hold values from -0.0625 to 0.0625
- kv_gain: float32 [512], replicated, may hold values from 0.25 to 1.75
- q_nope: bfloat16 [1024, 16384], P('seq', 'tensor'), may hold values from -90 to 90
- q_pe: bfloat16 [1024, 8192], P('seq', 'tensor'), may hold values from -6 to 6
- w_uk: bfloat16 [128, 128, 512], P('tensor'), may hold values from -0.5 to 0.5
- w_uv: bfloat16 [128, 512, 128], P('tensor'), may hold values from -1 to 1
- doc_ids: int32 [1024], replicated, may hold values from 0 to 3, never falling along the last dimension, each value on 1 to 768 neighbouring positions
- slot_table: int32 [64], replicated, may hold values from 0 to 63, each once
Outputs:
- attn_values: bfloat16 [1024, 16384], P('seq', 'tensor')
- latent_cache: bfloat16 [1024, 576], P('seq')
The draws below stay inside these ranges and needn't reach their ends.
Inputs may be any that keep to these rules, and one draw needn't show every extreme that they name: `doc_ids`: 4 documents packed in order, the longest exactly 768 tokens. `slot_table`: each cache slot receives exactly one token block.
All inputs are finite; a program needn't handle non-finite values.
Results may differ from the reference program's by a relative error of at most 0.0093.
Values may be sent and summed in bfloat16 or wider, within the bound.
A program may use at most 128 MiB of HBM per device.

```python
import functools
import math
import jax
import jax.numpy as jnp
import numpy as np
from jax import lax

D = 7168
HEADS = 128
LATENT = 512
ROPE = 64
NOPE = 128
VD = 128
BLOCK = 16
DOCS = 4
TOKENS = 1024


def draw_hidden(key, part):
    scale_key, column_key, entry_key = jax.random.split(jax.random.fold_in(key, 11), 3)
    row_scale = jnp.exp(jax.random.uniform(scale_key, (TOKENS, 1), jnp.float32, 0.0, math.log(10.0)))
    column_ramp = (1.0 + 2.5 * jnp.arange(D, dtype=jnp.float32) / D)[None, :]
    column_scale = column_ramp * jnp.exp(jax.random.uniform(column_key, (1, D), jnp.float32, -0.5, 0.5))
    gaussian = jax.random.normal(entry_key, (TOKENS, D), jnp.float32)
    return jnp.clip(gaussian * row_scale * column_scale, -200.0, 200.0).astype(jnp.bfloat16)


def draw_q_nope(key, part):
    entry_key = jax.random.fold_in(jax.random.fold_in(key, 23), 0)
    values = jnp.clip(jax.random.normal(entry_key, (TOKENS, HEADS * NOPE), jnp.float32), -6.0, 6.0)
    return values.astype(jnp.bfloat16)


def level_of(stream_key, dims, shards, least, largest):
    level, own = 1.0, jax.random.fold_in(stream_key, 6)
    for position, blocks in shards:
        heights = jnp.exp(jax.random.uniform(jax.random.fold_in(own, position), (blocks,), jnp.float32, least / len(shards), largest / len(shards)))
        level = level * jnp.repeat(heights, dims[position] // blocks).reshape([-1 if axis == position else 1 for axis in range(len(dims))])
    return level


def profile(amount, total, most, skew):
    weights = [(1 << 20) // math.isqrt(standing ** skew) + 1 for standing in range(2, amount + 1)]
    spare, counts = total - most - (amount - 1), [1] * (amount - 1)
    while spare > 0:
        candidates = [i for i in range(amount - 1) if counts[i] < most]
        mass, remaining = sum([weights[i] for i in candidates]), spare
        for i in candidates:
            more = min(most - counts[i], max(1, remaining * weights[i] // mass), spare)
            counts[i] = counts[i] + more
            spare = spare - more
    return np.array([most] + counts)


def ragged_sizes(rng, number_of, total, most, slope):
    if number_of == 2:
        one = jax.random.randint(rng, (), max(1, total - most), min(most, total - 1) + 1)
        return jnp.stack([one, total - one])
    tallies = jnp.asarray(profile(number_of, total, most, slope), jnp.int32)
    pairs = (number_of - 1) // 2
    source_of, taker = tallies[1:1 + 2 * pairs:2], tallies[2:2 + 2 * pairs:2]
    room = jnp.minimum(source_of - 1, most - taker)
    moved = jax.random.randint(jax.random.fold_in(rng, 1), (pairs,), 0, 1 << 20) % (room + 1)
    tallies = tallies.at[1:1 + 2 * pairs:2].set(source_of - moved).at[2:2 + 2 * pairs:2].set(taker + moved)
    return tallies[jax.random.permutation(jax.random.fold_in(rng, 2), number_of)]


def noise(own_key, dims, scale, bound, pieces=(), kind=jnp.bfloat16):
    array = scale * jax.random.normal(own_key, dims, jnp.float32)
    if pieces:
        array = array * level_of(own_key, dims, pieces, -0.22, 0.18)
    return jnp.clip(array, -bound, bound).astype(kind)


def setup_inputs(seed: int = 0) -> dict:
    splits = jax.random.split(jax.random.key(seed), 11)
    return {
        "hidden": draw_hidden(jax.random.fold_in(splits[10], 71), 0),
        "attn_gain": jnp.clip(1.0 + 0.15 * jax.random.normal(splits[1], (D,), jnp.float32), 0.25, 1.75),
        "kv_down": noise(splits[2], (D, LATENT + ROPE), D ** -0.5, 0.0625, ((0, 2),)),
        "kv_gain": jnp.clip(1.0 + 0.15 * jax.random.normal(splits[3], (LATENT,), jnp.float32), 0.25, 1.75),
        "q_nope": draw_q_nope(jax.random.fold_in(splits[10], 71), 0),
        "q_pe": noise(splits[5], (TOKENS, HEADS * ROPE), 1.0, 6.0, ((0, 16), (1, 2))),
        "w_uk": noise(splits[6], (HEADS, NOPE, LATENT), NOPE ** -0.5, 0.5, ((0, 2),)),
        "w_uv": noise(splits[7], (HEADS, LATENT, VD), (LATENT // 16) ** -0.5, 1.0, ((0, 2),)),
        "doc_ids": jnp.searchsorted(jnp.cumsum(ragged_sizes(splits[8], DOCS, TOKENS, TOKENS * 3 // 4, 0)), jnp.arange(TOKENS), side="right").astype(jnp.int32),
        "slot_table": jax.random.permutation(splits[9], TOKENS // BLOCK).astype(jnp.int32),
    }


EPSILON = 1e-06
MASKED = -1e+30

def rounded(value):
    return lax.optimization_barrier(value.astype(jnp.bfloat16))

def block_rows(total_rows):
    block_size = min(total_rows, 512)
    while total_rows % block_size:
        block_size -= 1
    return block_size

def angles(positions, width):
    middle = width // 2
    frequency = jnp.exp(jnp.arange(middle, dtype=jnp.float32) * (-2.0 * math.log(10000.0) / width))
    angle_table = positions[:, None] * frequency[None, :]
    return (jnp.cos(angle_table), jnp.sin(angle_table))

def rotate(values, cosine_part, sine_part):
    middle = values.shape[-1] // 2
    first_half = values[..., :middle]
    second_half = values[..., middle:]
    return jnp.concatenate([first_half * cosine_part - second_half * sine_part, second_half * cosine_part + first_half * sine_part], axis=-1)

def finish(projected, squares, positions, kv_gain):
    scaled = projected * lax.rsqrt(squares / D + EPSILON)[:, None]
    raw_latent = scaled[:, :LATENT]
    raw_key = scaled[:, LATENT:]
    latent = (raw_latent * lax.rsqrt(lax.optimization_barrier(jnp.mean(raw_latent * raw_latent, axis=1, keepdims=True)) + EPSILON) * kv_gain).astype(jnp.bfloat16)
    cosine_part, sine_part = angles(positions.astype(jnp.float32), raw_key.shape[1])
    return (latent, rotate(raw_key, cosine_part, sine_part).astype(jnp.bfloat16))

def attend_group(inputs, keys_latent, keys_rope, allowed):
    nope_group, rope_group, down_keys, up_values = inputs
    highest = lax.Precision.HIGHEST
    query_latent = rounded(jnp.einsum('thd,hdc->thc', nope_group.astype(jnp.float32), down_keys.astype(jnp.float32), precision=highest)).astype(jnp.float32)
    scores = jnp.einsum('thc,uc->thu', query_latent, keys_latent.astype(jnp.float32), precision=highest)
    scores = scores + jnp.einsum('thr,ur->thu', rope_group.astype(jnp.float32), keys_rope.astype(jnp.float32), precision=highest)
    scores = scores * (NOPE + ROPE) ** (-0.5)
    scores = jnp.where(allowed[:, None, :], scores, MASKED)
    top_score = lax.optimization_barrier(jnp.max(scores, axis=2, keepdims=True))
    weights = jnp.where(allowed[:, None, :], jnp.exp(scores - top_score), 0.0)
    denominator = lax.optimization_barrier(jnp.sum(weights, axis=2, keepdims=True))
    weighted = jnp.einsum('thu,uc->thc', rounded(weights).astype(jnp.float32), keys_latent.astype(jnp.float32), precision=highest)
    mixed = rounded(weighted / denominator).astype(jnp.float32)
    return jnp.einsum('thc,hcv->thv', mixed, up_values.astype(jnp.float32), precision=highest).astype(jnp.bfloat16)

def reference(hidden, attn_gain, kv_down, kv_gain, q_nope, q_pe, w_uk, w_uv, doc_ids, slot_table):
    widened = hidden.astype(jnp.float32)
    squares = lax.optimization_barrier(jnp.sum(widened * widened, axis=1))
    normed_in = (widened * attn_gain).astype(jnp.bfloat16)
    projected = jnp.dot(normed_in, kv_down, preferred_element_type=jnp.float32)
    positions = jnp.arange(TOKENS, dtype=jnp.int32)
    latent, key_rope = finish(projected, squares, positions, kv_gain)
    cosine_part, sine_part = angles(positions.astype(jnp.float32), ROPE)
    query_rope = rotate(q_pe.astype(jnp.float32).reshape(TOKENS, HEADS, ROPE), cosine_part[:, None, :], sine_part[:, None, :]).astype(jnp.bfloat16)
    query_rows = block_rows(TOKENS)
    group = 16 if HEADS % 16 == 0 else HEADS
    groups = HEADS // group
    down_groups = w_uk.reshape(groups, group, NOPE, LATENT)
    up_groups = w_uv.reshape(groups, group, LATENT, VD)
    outputs = []
    for block_index in range(TOKENS // query_rows):
        begin = block_index * query_rows
        end = begin + query_rows
        allowed = (positions[None, :end] <= positions[begin:end, None]) & (doc_ids[None, :end] == doc_ids[begin:end, None])
        nope_part = q_nope[begin:end].reshape(query_rows, groups, group, NOPE).transpose(1, 0, 2, 3)
        rope_part = query_rope[begin:end].reshape(query_rows, groups, group, ROPE).transpose(1, 0, 2, 3)
        attend = functools.partial(attend_group, keys_latent=latent[:end], keys_rope=key_rope[:end], allowed=allowed)
        result = lax.map(attend, (nope_part, rope_part, down_groups, up_groups))
        outputs.append(result.transpose(1, 0, 2, 3).reshape(query_rows, HEADS * VD))
    attn_values = jnp.concatenate(outputs, axis=0)
    blocks = jnp.concatenate([latent, key_rope], axis=1).reshape(TOKENS // BLOCK, BLOCK, LATENT + ROPE)
    latent_cache = jnp.zeros_like(blocks).at[slot_table].set(blocks).reshape(TOKENS, LATENT + ROPE)
    return (attn_values, latent_cache)
```

```python
import functools
import math

import jax
import jax.numpy as jnp
import numpy as np
from jax import lax
from jax.experimental import pallas as pl
from jax.experimental.pallas import tpu as pltpu
from jax.sharding import PartitionSpec as P

LATENT = 512
ROPE = 64
NOPE = 128
VD = 128
BLOCK = 16
LANES = 128
EPSILON = 1e-06
MASKED = -1e30
WIDE = LATENT + 2 * ROPE
VMEM_BYTES = 56 * 1024 * 1024
MESH = pl.DeviceIdType.MESH


def rope_table(tokens):
    middle = ROPE // 2
    frequency = np.exp(np.arange(middle, dtype=np.float32) * np.float32(-2.0 * math.log(10000.0) / ROPE)).astype(np.float32)
    angle = (np.arange(tokens, dtype=np.float32)[:, None] * frequency[None, :]).astype(np.float32)
    cosine, sine = np.cos(angle), np.sin(angle)
    return np.concatenate([cosine] * 4 + [-sine, sine, -sine, sine], axis=1).astype(np.float32)


def rotate_pair(values, cosine, sine, lane):
    half = ROPE // 2
    swapped = jnp.where(
        lane % ROPE < half,
        pltpu.roll(values, LANES - half, 1),
        pltpu.roll(values, half, 1),
    )
    return values * cosine + swapped * sine


def gather_kernel(
    nseq, width,
    hidden, gain, kv_down, kv_gain, q_nope, q_pe, w_uk, table,
    qc_out, kv_out,
    hidden_v, gain_v, down_v, kv_gain_v, nope_v, pe_v, uk_v, table_v,
    partial, incoming, kv, qc,
    in_sem, down_sem, uk_sem, out_sem, x_send, x_recv, send_sem, recv_sem,
):
    rows, model = hidden_v.shape
    heads = uk_v.shape[0]
    half = rows // 2
    groups = nseq // 4
    me = lax.axis_index("seq")
    side = lax.axis_index("tensor")
    far = me // 4
    place = lax.rem(me, 4)
    ybit = place // 2
    core = lax.rem(place, 2)

    first_row = pl.multiple_of(me * rows, rows)
    early = [
        pltpu.make_async_copy(hidden, hidden_v, in_sem.at[0]),
        pltpu.make_async_copy(gain, gain_v, in_sem.at[1]),
        pltpu.make_async_copy(kv_gain, kv_gain_v, in_sem.at[2]),
        pltpu.make_async_copy(table.at[pl.ds(first_row, rows)], table_v, in_sem.at[3]),
    ]
    for copy in early[:2]:
        copy.start()
    chunks = down_sem.shape[0]
    depth = model // chunks
    down_copies = []
    for i in range(chunks):
        part = pl.ds(i * depth, depth)
        down_copies.append(pltpu.make_async_copy(kv_down.at[part], down_v.at[part], down_sem.at[i]))
        down_copies[-1].start()
    for copy in early[2:]:
        copy.start()
    query_copies = [
        pltpu.make_async_copy(q_nope, nope_v, in_sem.at[4]),
        pltpu.make_async_copy(q_pe, pe_v, in_sem.at[5]),
    ]
    for copy in query_copies:
        copy.start()
    stages = uk_sem.shape[0]
    stage_heads = heads // stages
    uk_copies = []
    for i in range(stages):
        part = pl.ds(i * stage_heads, stage_heads)
        uk_copies.append(pltpu.make_async_copy(w_uk.at[part], uk_v.at[part], uk_sem.at[i]))
        uk_copies[-1].start()

    def peer(seq, tensor):
        return {"seq": seq, "tensor": tensor}

    def seq_of(group, y, c):
        return group * 4 + y * 2 + c

    x_peer = peer(me, 1 - side)
    y_peer = peer(seq_of(far, 1 - ybit, core), side)
    core_peer = peer(seq_of(far, ybit, 1 - core), side)
    z_groups = [lax.rem(far + k, groups) for k in range(1, groups)]
    z_peers = [peer(seq_of(g, ybit, core), side) for g in z_groups]

    barrier = pltpu.get_barrier_semaphore()
    everyone = [x_peer, y_peer, core_peer] + z_peers
    for target in everyone:
        pl.semaphore_signal(barrier, inc=1, device_id=target, device_id_type=MESH)

    for copy in early[:2]:
        copy.wait()
    squares = jnp.zeros((rows, 1), jnp.float32)
    total = jnp.zeros((rows, width), jnp.float32)
    for i in range(chunks):
        part = pl.ds(i * depth, depth)
        widened = hidden_v[:, part].astype(jnp.float32)
        squares = squares + jnp.sum(widened * widened, axis=1, keepdims=True)
        normed = (widened * gain_v[:, part]).astype(jnp.bfloat16)
        down_copies[i].wait()
        total = total + jnp.dot(normed, down_v[part, :], preferred_element_type=jnp.float32)
    partial[:, pl.ds(0, width)] = total
    partial[:, pl.ds(width, WIDE - width)] = jnp.broadcast_to(squares, (rows, WIDE - width))
    pl.semaphore_wait(barrier, len(everyone))
    theirs = pl.multiple_of((1 - side) * half, half)
    ours = pl.multiple_of(side * half, half)
    x_copy = pltpu.make_async_remote_copy(
        src_ref=partial.at[pl.ds(theirs, half)],
        dst_ref=incoming,
        send_sem=x_send.at[0],
        recv_sem=x_recv.at[0],
        device_id=x_peer,
        device_id_type=MESH,
    )
    x_copy.start()

    lane = lax.broadcasted_iota(jnp.int32, (1, LANES), 1)
    for copy in early[2:] + query_copies:
        copy.wait()
    out_copies = []

    def queries(stage):
        uk_copies[stage].wait()

        def pair(index, carry):
            head = index * 2
            at = pl.multiple_of(index * LANES, LANES)
            turned = rotate_pair(
                pe_v[:, pl.ds(at, LANES)].astype(jnp.float32),
                table_v[:, :LANES], table_v[:, LANES:], lane,
            )
            for j in range(2):
                column = pl.multiple_of((head + j) * NOPE, NOPE)
                qc[head + j, :, pl.ds(0, LATENT)] = jnp.dot(
                    nope_v[:, pl.ds(column, NOPE)], uk_v[head + j],
                    preferred_element_type=jnp.float32,
                ).astype(jnp.bfloat16)
                mine = (lane < ROPE) if j == 0 else (lane >= ROPE)
                qc[head + j, :, pl.ds(LATENT, LANES)] = jnp.where(mine, turned, 0.0).astype(jnp.bfloat16)
            return carry

        lax.fori_loop(stage * stage_heads // 2, (stage + 1) * stage_heads // 2, pair, 0, unroll=2)
        part = pl.ds(stage * stage_heads, stage_heads)
        copy = pltpu.make_async_copy(qc.at[part], qc_out.at[part], out_sem.at[stage])
        copy.start()
        out_copies.append(copy)

    queries(0)
    queries(1)

    x_copy.wait()
    summed = partial[pl.ds(ours, half), :] + incoming[...]
    norm = lax.rsqrt(summed[:, width:width + 1] / (2 * model) + EPSILON)
    raw = summed[:, :LATENT] * norm
    mean = jnp.sum(raw * raw, axis=1, keepdims=True) * (1.0 / LATENT)
    latent = raw * lax.rsqrt(mean + EPSILON) * kv_gain_v[...]
    tail = summed[:, LATENT:] * norm
    doubled = jnp.where(lane < ROPE, tail, pltpu.roll(tail, ROPE, 1))
    turned = rotate_pair(
        doubled, table_v[pl.ds(ours, half), :LANES], table_v[pl.ds(ours, half), LANES:], lane
    )

    def rows_of(seq, tensor):
        return pl.ds(pl.multiple_of(seq * rows + tensor * half, half), half)

    own = rows_of(me, side)
    kv[own, pl.ds(0, LATENT)] = latent.astype(jnp.bfloat16)
    kv[own, pl.ds(LATENT, LANES)] = turned.astype(jnp.bfloat16)

    sent = []

    def chunk(seq, tensor):
        return seq * 2 + tensor

    def send(seq, tensor, target):
        span = rows_of(seq, tensor)
        copy = pltpu.make_async_remote_copy(
            src_ref=kv.at[span],
            dst_ref=kv.at[span],
            send_sem=send_sem.at[len(sent)],
            recv_sem=recv_sem.at[chunk(seq, tensor)],
            device_id=target,
            device_id_type=MESH,
        )
        copy.start()
        sent.append(copy)

    def arrive(seq, tensor):
        span = rows_of(seq, tensor)
        pltpu.make_async_remote_copy(
            src_ref=kv.at[span],
            dst_ref=kv.at[span],
            send_sem=send_sem.at[0],
            recv_sem=recv_sem.at[chunk(seq, tensor)],
            device_id=x_peer,
            device_id_type=MESH,
        ).wait_recv()

    for target in z_peers:
        send(me, side, target)
    send(me, side, x_peer)
    send(me, side, y_peer)
    send(me, side, core_peer)
    queries(2)
    for g in z_groups:
        s = seq_of(g, ybit, core)
        arrive(s, side)
        send(s, side, x_peer)
        send(s, side, y_peer)
        send(s, side, core_peer)
    queries(3)
    for k in range(groups):
        g = lax.rem(far + k, groups)
        s = seq_of(g, ybit, core)
        arrive(s, 1 - side)
        if k % 2 == 0:
            send(s, 1 - side, y_peer)
        send(s, 1 - side, core_peer)
        s = seq_of(g, 1 - ybit, core)
        arrive(s, side)
        if k % 2 == 1:
            send(s, side, x_peer)
        send(s, side, core_peer)
    for k in range(groups):
        s = seq_of(lax.rem(far + k, groups), 1 - ybit, core)
        arrive(s, 1 - side)
        send(s, 1 - side, core_peer)
    for k in range(groups):
        g = lax.rem(far + k, groups)
        for y in range(2):
            for t in range(2):
                arrive(seq_of(g, y, 1 - core), t)
    last = pltpu.make_async_copy(kv, kv_out, out_sem.at[stages])
    last.start()
    for copy in sent:
        copy.wait_send()
    for copy in out_copies:
        copy.wait()
    last.wait()


def attend_kernel(sub, slots, qc, uv, kv, docs, out, cache, bias):
    heads, rows, _ = qc.shape
    tokens = kv.shape[0]
    me = lax.axis_index("seq")
    first_row = me * rows

    @pl.when(pl.program_id(0) == 0)
    def _():
        key = lax.broadcasted_iota(jnp.int32, (rows, tokens), 1)
        query = first_row + lax.broadcasted_iota(jnp.int32, (rows, tokens), 0)
        key_doc = jnp.broadcast_to(docs[...], (rows, tokens))
        query_doc = jnp.sum(
            jnp.where(key == query, key_doc, 0).astype(jnp.float32), axis=1, keepdims=True
        )
        allowed = (key <= query) & (key_doc.astype(jnp.float32) == query_doc)
        bias[...] = jnp.where(allowed, 0.0, MASKED)
        per = rows // BLOCK

        def place(block, carry):
            slot = slots[block]

            @pl.when(slot // per == me)
            def _():
                to = pl.ds(pl.multiple_of(lax.rem(slot, per) * BLOCK, BLOCK), BLOCK)
                source = pl.ds(pl.multiple_of(block * BLOCK, BLOCK), BLOCK)
                cache[to, :] = kv[source, pl.ds(0, cache.shape[1])]

            return carry

        lax.fori_loop(0, tokens // BLOCK, place, 0)

    scale = (NOPE + ROPE) ** (-0.5) * math.log2(math.e)
    for start in range(0, heads, sub):
        query = qc[pl.ds(start, sub)].reshape(sub * rows, WIDE)
        scores = lax.dot_general(
            query, kv[...], (((1,), (1,)), ((), ())), preferred_element_type=jnp.float32
        )
        scores = (scores.reshape(sub, rows, tokens) + bias[...][None]).reshape(sub * rows, tokens)
        top = jnp.max(scores, axis=1, keepdims=True)
        weights = jnp.exp2((scores - top) * scale)
        denominator = jnp.sum(weights, axis=1, keepdims=True)
        mixed = jnp.dot(
            weights.astype(jnp.bfloat16), kv[:, pl.ds(0, LATENT)], preferred_element_type=jnp.float32
        )
        mixed = (mixed / denominator).astype(jnp.bfloat16)
        for j in range(sub):
            out[:, pl.ds((start + j) * VD, VD)] = jnp.dot(
                mixed[j * rows:(j + 1) * rows], uv[start + j], preferred_element_type=jnp.float32
            ).astype(jnp.bfloat16)


def local(nseq, hidden, attn_gain, kv_down, kv_gain, q_nope, q_pe, w_uk, w_uv, doc_ids, slot_table):
    rows, model = hidden.shape
    width = kv_down.shape[1]
    heads = w_uk.shape[0]
    tokens = doc_ids.shape[0]
    table = jnp.asarray(rope_table(tokens))
    stages = 4
    anywhere = pl.BlockSpec(memory_space=pl.ANY)
    dma = pltpu.SemaphoreType.DMA
    groups = nseq // 4
    sends = (groups + 2) + (groups - 1) * 3 + groups * 3 + groups
    qc, kv = pl.pallas_call(
        functools.partial(gather_kernel, nseq, width),
        out_shape=(
            jax.ShapeDtypeStruct((heads, rows, WIDE), jnp.bfloat16),
            jax.ShapeDtypeStruct((tokens, WIDE), jnp.bfloat16),
        ),
        in_specs=[anywhere] * 8,
        out_specs=(anywhere, anywhere),
        scratch_shapes=[
            pltpu.VMEM((rows, model), jnp.bfloat16),
            pltpu.VMEM((1, model), jnp.float32),
            pltpu.VMEM((model, width), jnp.bfloat16),
            pltpu.VMEM((1, LATENT), jnp.float32),
            pltpu.VMEM((rows, heads * NOPE), jnp.bfloat16),
            pltpu.VMEM((rows, heads * ROPE), jnp.bfloat16),
            pltpu.VMEM((heads, NOPE, LATENT), jnp.bfloat16),
            pltpu.VMEM((rows, 2 * LANES), jnp.float32),
            pltpu.VMEM((rows, WIDE), jnp.float32),
            pltpu.VMEM((rows // 2, WIDE), jnp.float32),
            pltpu.VMEM((tokens, WIDE), jnp.bfloat16),
            pltpu.VMEM((heads, rows, WIDE), jnp.bfloat16),
            dma((6,)),
            dma((7,)),
            dma((stages,)),
            dma((stages + 1,)),
            dma((1,)),
            dma((1,)),
            dma((sends,)),
            dma((2 * nseq,)),
        ],
        compiler_params=pltpu.CompilerParams(
            collective_id=0, has_side_effects=True, vmem_limit_bytes=VMEM_BYTES
        ),
        name="gather",
    )(
        hidden, attn_gain.reshape(1, model), kv_down, kv_gain.reshape(1, LATENT),
        q_nope, q_pe, w_uk, table,
    )
    group = 8
    return pl.pallas_call(
        functools.partial(attend_kernel, 4),
        out_shape=(
            jax.ShapeDtypeStruct((rows, heads * VD), jnp.bfloat16),
            jax.ShapeDtypeStruct((rows, width), jnp.bfloat16),
        ),
        grid_spec=pltpu.PrefetchScalarGridSpec(
            num_scalar_prefetch=1,
            grid=(heads // group,),
            in_specs=[
                pl.BlockSpec((group, rows, WIDE), lambda i, s: (i, 0, 0)),
                pl.BlockSpec((group, LATENT, VD), lambda i, s: (i, 0, 0)),
                pl.BlockSpec((tokens, WIDE), lambda i, s: (0, 0)),
                pl.BlockSpec((1, tokens), lambda i, s: (0, 0)),
            ],
            out_specs=[
                pl.BlockSpec((rows, group * VD), lambda i, s: (0, i)),
                pl.BlockSpec((rows, width), lambda i, s: (0, 0)),
            ],
            scratch_shapes=[pltpu.VMEM((rows, tokens), jnp.float32)],
        ),
        compiler_params=pltpu.CompilerParams(
            dimension_semantics=("arbitrary",), vmem_limit_bytes=VMEM_BYTES
        ),
        name="attend",
    )(slot_table, qc, w_uv, kv, doc_ids.reshape(1, tokens))


def solution(mesh):
    placed = (
        P("seq", "tensor"),
        P("tensor"),
        P("tensor", None),
        P(),
        P("seq", "tensor"),
        P("seq", "tensor"),
        P("tensor", None, None),
        P("tensor", None, None),
        P(),
        P(),
    )
    return jax.shard_map(
        functools.partial(local, mesh.shape["seq"]),
        mesh=mesh,
        in_specs=placed,
        out_specs=(P("seq", "tensor"), P("seq", None)),
        check_vma=False,
    )
```

```python
import functools
import math

import jax
import jax.numpy as jnp
import numpy as np
from jax import lax
from jax.experimental import pallas as pl
from jax.experimental.pallas import tpu as pltpu
from jax.sharding import PartitionSpec as P

LATENT = 512
ROPE = 64
NOPE = 128
VD = 128
BLOCK = 16
LANES = 128
EPSILON = 1e-06
MASKED = -1e30
WIDE = LATENT + 2 * ROPE
VMEM_BYTES = 56 * 1024 * 1024
MESH = pl.DeviceIdType.MESH
WINDOWS = (2, 4, 6, 7, 8)
GROUP = 8
SUB = 4


def rope_table(tokens):
    middle = ROPE // 2
    frequency = np.exp(np.arange(middle, dtype=np.float32) * np.float32(-2.0 * math.log(10000.0) / ROPE)).astype(np.float32)
    angle = (np.arange(tokens, dtype=np.float32)[:, None] * frequency[None, :]).astype(np.float32)
    cosine, sine = np.cos(angle), np.sin(angle)
    return np.concatenate([cosine] * 4 + [-sine, sine, -sine, sine], axis=1).astype(np.float32)


def rotate_pair(values, cosine, sine, lane):
    half = ROPE // 2
    swapped = jnp.where(
        lane % ROPE < half,
        pltpu.roll(values, LANES - half, 1),
        pltpu.roll(values, half, 1),
    )
    return values * cosine + swapped * sine


def gather_kernel(
    nseq, width,
    hidden, gain, kv_down, kv_gain, q_nope, q_pe, w_uk, table,
    qc_out, kv_out,
    hidden_v, gain_v, down_v, kv_gain_v, nope_v, pe_v, uk_v, table_v,
    partial, incoming, kv, qc,
    in_sem, down_sem, uk_sem, out_sem, x_send, x_recv, send_sem, recv_sem,
):
    rows, model = hidden_v.shape
    heads = uk_v.shape[0]
    half = rows // 2
    groups = nseq // 4
    me = lax.axis_index("seq")
    side = lax.axis_index("tensor")
    far = me // 4
    place = lax.rem(me, 4)
    ybit = place // 2
    core = lax.rem(place, 2)

    first_row = pl.multiple_of(me * rows, rows)
    early = [
        pltpu.make_async_copy(hidden, hidden_v, in_sem.at[0]),
        pltpu.make_async_copy(gain, gain_v, in_sem.at[1]),
        pltpu.make_async_copy(kv_gain, kv_gain_v, in_sem.at[2]),
        pltpu.make_async_copy(table.at[pl.ds(first_row, rows)], table_v, in_sem.at[3]),
    ]
    for copy in early[:2]:
        copy.start()
    chunks = down_sem.shape[0]
    depth = model // chunks
    down_copies = []
    for i in range(chunks):
        part = pl.ds(i * depth, depth)
        down_copies.append(
            pltpu.make_async_copy(kv_down.at[:, part], down_v.at[:, part], down_sem.at[i])
        )
        down_copies[-1].start()
    for copy in early[2:]:
        copy.start()
    query_copies = [
        pltpu.make_async_copy(q_nope, nope_v, in_sem.at[4]),
        pltpu.make_async_copy(q_pe, pe_v, in_sem.at[5]),
    ]
    for copy in query_copies:
        copy.start()
    stages = uk_sem.shape[0]
    stage_heads = heads // stages
    uk_copies = []
    for i in range(stages):
        part = pl.ds(i * stage_heads, stage_heads)
        uk_copies.append(pltpu.make_async_copy(w_uk.at[part], uk_v.at[part], uk_sem.at[i]))
        uk_copies[-1].start()

    def peer(seq, tensor):
        return {"seq": seq, "tensor": tensor}

    def seq_of(group, y, c):
        return group * 4 + y * 2 + c

    x_peer = peer(me, 1 - side)
    y_peer = peer(seq_of(far, 1 - ybit, core), side)
    core_peer = peer(seq_of(far, ybit, 1 - core), side)
    upper = far // ((groups + 1) // 2)
    step = 1 - 2 * upper
    inward = far + upper * (groups - 1 - 2 * far)
    hops = [1, 2 + inward, 3 - inward] if groups == 4 else list(range(1, groups))
    z_groups = [lax.rem(far + step * hop + groups, groups) for hop in hops]
    z_peers = [peer(seq_of(g, ybit, core), side) for g in z_groups]

    barrier = pltpu.get_barrier_semaphore()
    everyone = [x_peer, y_peer, core_peer] + z_peers
    for target in everyone:
        pl.semaphore_signal(barrier, inc=1, device_id=target, device_id_type=MESH)

    for copy in early[:2]:
        copy.wait()
    squares = jnp.zeros((rows, 1), jnp.float32)
    total = jnp.zeros((rows, width), jnp.float32)
    for i in range(chunks):
        part = pl.ds(i * depth, depth)
        widened = hidden_v[:, part].astype(jnp.float32)
        squares = squares + jnp.sum(widened * widened, axis=1, keepdims=True)
        normed = (widened * gain_v[part].reshape(1, depth)).astype(jnp.bfloat16)
        down_copies[i].wait()
        total = total + lax.dot_general(
            normed, down_v[:, part], (((1,), (1,)), ((), ())), preferred_element_type=jnp.float32
        )
    partial[:, pl.ds(0, width)] = total
    partial[:, pl.ds(width, WIDE - width)] = jnp.broadcast_to(squares, (rows, WIDE - width))
    pl.semaphore_wait(barrier, len(everyone))
    theirs = pl.multiple_of((1 - side) * half, half)
    ours = pl.multiple_of(side * half, half)
    x_copy = pltpu.make_async_remote_copy(
        src_ref=partial.at[pl.ds(theirs, half)],
        dst_ref=incoming,
        send_sem=x_send.at[0],
        recv_sem=x_recv.at[0],
        device_id=x_peer,
        device_id_type=MESH,
    )
    x_copy.start()

    lane = lax.broadcasted_iota(jnp.int32, (1, LANES), 1)
    for copy in early[2:] + query_copies:
        copy.wait()
    out_copies = []

    def queries(stage):
        uk_copies[stage].wait()

        def pair(index, carry):
            head = index * 2
            at = pl.multiple_of(index * LANES, LANES)
            turned = rotate_pair(
                pe_v[:, pl.ds(at, LANES)].astype(jnp.float32),
                table_v[:, :LANES], table_v[:, LANES:], lane,
            )
            for j in range(2):
                column = pl.multiple_of((head + j) * NOPE, NOPE)
                qc[head + j, :, pl.ds(0, LATENT)] = jnp.dot(
                    nope_v[:, pl.ds(column, NOPE)], uk_v[head + j],
                    preferred_element_type=jnp.float32,
                ).astype(jnp.bfloat16)
                mine = (lane < ROPE) if j == 0 else (lane >= ROPE)
                qc[head + j, :, pl.ds(LATENT, LANES)] = jnp.where(mine, turned, 0.0).astype(jnp.bfloat16)
            return carry

        lax.fori_loop(stage * stage_heads // 2, (stage + 1) * stage_heads // 2, pair, 0, unroll=2)
        part = pl.ds(stage * stage_heads, stage_heads)
        copy = pltpu.make_async_copy(qc.at[part], qc_out.at[part], out_sem.at[stage])
        copy.start()
        out_copies.append(copy)

    queries(0)
    queries(1)

    x_copy.wait()
    summed = partial[pl.ds(ours, half), :] + incoming[...]
    norm = lax.rsqrt(summed[:, width:width + 1] / (2 * model) + EPSILON)
    raw = summed[:, :LATENT] * norm
    mean = jnp.sum(raw * raw, axis=1, keepdims=True) * (1.0 / LATENT)
    latent = raw * lax.rsqrt(mean + EPSILON) * kv_gain_v[...]
    tail = summed[:, LATENT:] * norm
    doubled = jnp.where(lane < ROPE, tail, pltpu.roll(tail, ROPE, 1))
    turned = rotate_pair(
        doubled, table_v[pl.ds(ours, half), :LANES], table_v[pl.ds(ours, half), LANES:], lane
    )

    def rows_of(seq, tensor):
        return pl.ds(pl.multiple_of(seq * rows + tensor * half, half), half)

    own = rows_of(me, side)
    kv[own, pl.ds(0, LATENT)] = latent.astype(jnp.bfloat16)
    kv[own, pl.ds(LATENT, LANES)] = turned.astype(jnp.bfloat16)

    sent = []

    def chunk(seq, tensor):
        return seq * 2 + tensor

    def send(seq, tensor, target):
        span = rows_of(seq, tensor)
        copy = pltpu.make_async_remote_copy(
            src_ref=kv.at[span],
            dst_ref=kv.at[span],
            send_sem=send_sem.at[len(sent)],
            recv_sem=recv_sem.at[chunk(seq, tensor)],
            device_id=target,
            device_id_type=MESH,
        )
        copy.start()
        sent.append(copy)

    def arrive(seq, tensor):
        span = rows_of(seq, tensor)
        pltpu.make_async_remote_copy(
            src_ref=kv.at[span],
            dst_ref=kv.at[span],
            send_sem=send_sem.at[0],
            recv_sem=recv_sem.at[chunk(seq, tensor)],
            device_id=x_peer,
            device_id_type=MESH,
        ).wait_recv()

    for target in z_peers:
        send(me, side, target)
    send(me, side, x_peer)
    send(me, side, y_peer)
    send(me, side, core_peer)
    queries(2)
    for g in z_groups:
        s = seq_of(g, ybit, core)
        arrive(s, side)
        send(s, side, x_peer)
        send(s, side, y_peer)
        send(s, side, core_peer)
    queries(3)
    for k, g in enumerate([far] + z_groups):
        s = seq_of(g, ybit, core)
        arrive(s, 1 - side)
        if k % 2 == 0:
            send(s, 1 - side, y_peer)
        send(s, 1 - side, core_peer)
        s = seq_of(g, 1 - ybit, core)
        arrive(s, side)
        if k % 2 == 1:
            send(s, side, x_peer)
        send(s, side, core_peer)
    for g in [far] + z_groups:
        s = seq_of(g, 1 - ybit, core)
        arrive(s, 1 - side)
        send(s, 1 - side, core_peer)
    for g in [far] + z_groups:
        for y in range(2):
            for t in range(2):
                arrive(seq_of(g, y, 1 - core), t)
    last = pltpu.make_async_copy(kv, kv_out, out_sem.at[stages])
    last.start()
    for copy in sent:
        copy.wait_send()
    for copy in out_copies:
        copy.wait()
    last.wait()


def attend_kernel(sub, slots, qc, uv, kv, docs, out, cache, bias, bounds):
    heads, rows, _ = qc.shape
    tokens = kv.shape[0]
    me = lax.axis_index("seq")
    first_row = me * rows
    sizes = [tokens * n // 8 for n in WINDOWS]

    @pl.when(pl.program_id(0) == 0)
    def _():
        key = lax.broadcasted_iota(jnp.int32, (1, tokens), 1)
        first_doc = jnp.sum(jnp.where(key == first_row, docs[...], 0).astype(jnp.float32), axis=1, keepdims=True)
        start = jnp.sum((docs[...].astype(jnp.float32) < first_doc).astype(jnp.float32)).astype(jnp.int32)
        needed = first_row + rows - start
        choice = jnp.int32(0)
        size = jnp.int32(sizes[0])
        for i in range(1, len(sizes)):
            more = needed > sizes[i - 1]
            choice = jnp.where(more, i, choice)
            size = jnp.where(more, sizes[i], size)
        window = jnp.maximum(first_row + rows - size, 0)
        bounds[0] = choice
        bounds[1] = window
        wide = (rows, tokens)
        at = lax.broadcasted_iota(jnp.int32, wide, 1)
        query = first_row + lax.broadcasted_iota(jnp.int32, wide, 0)
        every_doc = jnp.broadcast_to(docs[...].astype(jnp.float32), wide)
        query_doc = jnp.sum(jnp.where(at == query, every_doc, 0.0), axis=1, keepdims=True)
        lowest = jnp.sum((every_doc < query_doc).astype(jnp.float32), axis=1, keepdims=True)
        position = window + at
        allowed = (position <= query) & (position.astype(jnp.float32) >= lowest)
        bias[...] = jnp.where(allowed, 0.0, MASKED)
        per = rows // BLOCK

        def place(block, carry):
            slot = slots[block]

            @pl.when(slot // per == me)
            def _():
                to = pl.ds(pl.multiple_of(lax.rem(slot, per) * BLOCK, BLOCK), BLOCK)
                source = pl.ds(pl.multiple_of(block * BLOCK, BLOCK), BLOCK)
                cache[to, :] = kv[source, pl.ds(0, cache.shape[1])]

            return carry

        lax.fori_loop(0, tokens // BLOCK, place, 0)

    scale = (NOPE + ROPE) ** (-0.5) * math.log2(math.e)
    window = pl.multiple_of(bounds[1], rows)

    def attend(size):
        span = pl.ds(window, size)

        def score(start):
            query = qc[pl.ds(start, sub)].reshape(sub * rows, WIDE)
            return lax.dot_general(
                query, kv[span, :], (((1,), (1,)), ((), ())), preferred_element_type=jnp.float32
            )

        scores = score(0)
        for start in range(0, heads, sub):
            following = score(start + sub) if start + sub < heads else None
            scores = (scores.reshape(sub, rows, size) + bias[:, :size][None]).reshape(sub * rows, size)
            top = jnp.max(scores, axis=1, keepdims=True)
            weights = jnp.exp2((scores - top) * scale)
            denominator = jnp.sum(weights, axis=1, keepdims=True)
            mixed = jnp.dot(
                weights.astype(jnp.bfloat16), kv[span, pl.ds(0, LATENT)], preferred_element_type=jnp.float32
            )
            mixed = (mixed / denominator).astype(jnp.bfloat16)
            for j in range(sub):
                out[:, pl.ds((start + j) * VD, VD)] = jnp.dot(
                    mixed[j * rows:(j + 1) * rows], uv[start + j], preferred_element_type=jnp.float32
                ).astype(jnp.bfloat16)
            scores = following

    for i, size in enumerate(sizes):
        @pl.when(bounds[0] == i)
        def _(size=size):
            attend(size)


def local(nseq, hidden, attn_gain, kv_down, kv_gain, q_nope, q_pe, w_uk, w_uv, doc_ids, slot_table):
    rows, model = hidden.shape
    width = kv_down.shape[1]
    heads = w_uk.shape[0]
    tokens = doc_ids.shape[0]
    table = jnp.asarray(rope_table(tokens))
    stages = 4
    anywhere = pl.BlockSpec(memory_space=pl.ANY)
    dma = pltpu.SemaphoreType.DMA
    groups = nseq // 4
    sends = (groups + 2) + (groups - 1) * 3 + groups * 3 + groups
    qc, kv = pl.pallas_call(
        functools.partial(gather_kernel, nseq, width),
        out_shape=(
            jax.ShapeDtypeStruct((heads, rows, WIDE), jnp.bfloat16),
            jax.ShapeDtypeStruct((tokens, WIDE), jnp.bfloat16),
        ),
        in_specs=[anywhere] * 8,
        out_specs=(anywhere, anywhere),
        scratch_shapes=[
            pltpu.VMEM((rows, model), jnp.bfloat16),
            pltpu.VMEM((model,), jnp.float32),
            pltpu.VMEM((width, model), jnp.bfloat16),
            pltpu.VMEM((1, LATENT), jnp.float32),
            pltpu.VMEM((rows, heads * NOPE), jnp.bfloat16),
            pltpu.VMEM((rows, heads * ROPE), jnp.bfloat16),
            pltpu.VMEM((heads, NOPE, LATENT), jnp.bfloat16),
            pltpu.VMEM((rows, 2 * LANES), jnp.float32),
            pltpu.VMEM((rows, WIDE), jnp.float32),
            pltpu.VMEM((rows // 2, WIDE), jnp.float32),
            pltpu.VMEM((tokens, WIDE), jnp.bfloat16),
            pltpu.VMEM((heads, rows, WIDE), jnp.bfloat16),
            dma((6,)),
            dma((7,)),
            dma((stages,)),
            dma((stages + 1,)),
            dma((1,)),
            dma((1,)),
            dma((sends,)),
            dma((2 * nseq,)),
        ],
        compiler_params=pltpu.CompilerParams(
            collective_id=0, has_side_effects=True, vmem_limit_bytes=VMEM_BYTES
        ),
        name="gather",
    )(
        hidden, attn_gain, kv_down.T, kv_gain.reshape(1, LATENT),
        q_nope, q_pe, w_uk, table,
    )
    group = GROUP
    return pl.pallas_call(
        functools.partial(attend_kernel, SUB),
        out_shape=(
            jax.ShapeDtypeStruct((rows, heads * VD), jnp.bfloat16),
            jax.ShapeDtypeStruct((rows, width), jnp.bfloat16),
        ),
        grid_spec=pltpu.PrefetchScalarGridSpec(
            num_scalar_prefetch=1,
            grid=(heads // group,),
            in_specs=[
                pl.BlockSpec((group, rows, WIDE), lambda i, s: (i, 0, 0)),
                pl.BlockSpec((group, LATENT, VD), lambda i, s: (i, 0, 0)),
                pl.BlockSpec((tokens, WIDE), lambda i, s: (0, 0)),
                pl.BlockSpec((1, tokens), lambda i, s: (0, 0)),
            ],
            out_specs=[
                pl.BlockSpec((rows, group * VD), lambda i, s: (0, i)),
                pl.BlockSpec((rows, width), lambda i, s: (0, 0)),
            ],
            scratch_shapes=[pltpu.VMEM((rows, tokens), jnp.float32), pltpu.SMEM((2,), jnp.int32)],
        ),
        compiler_params=pltpu.CompilerParams(
            dimension_semantics=("arbitrary",), vmem_limit_bytes=VMEM_BYTES
        ),
        name="attend",
    )(slot_table, qc, w_uv, kv, doc_ids.reshape(1, tokens))


def solution(mesh):
    placed = (
        P("seq", "tensor"),
        P("tensor"),
        P("tensor", None),
        P(),
        P("seq", "tensor"),
        P("seq", "tensor"),
        P("tensor", None, None),
        P("tensor", None, None),
        P(),
        P(),
    )
    return jax.shard_map(
        functools.partial(local, mesh.shape["seq"]),
        mesh=mesh,
        in_specs=placed,
        out_specs=(P("seq", "tensor"), P("seq", None)),
        check_vma=False,
    )
```
